32 devices in a mesh: dp: 4 (over y, x), sp: 4 (over z), shift: 2 (over core).
Axes of the slice: x: 2, y: 2, z: 4, core: 2. Of those that a mesh axis runs over, the one named last changes fastest.
Arguments:
- query_rows: bfloat16 [8, 1024, 32, 128], P(('shift', 'dp'), 'sp'), parts along dimension 0, may hold values from -6 to 6
- key_rows: bfloat16 [8, 1024, 32, 128], P(('shift', 'dp'), 'sp'), parts along dimension 0, may hold values from -6 to 6
- value_rows: bfloat16 [8, 1024, 32, 128], P(('shift', 'dp'), 'sp'), parts along dimension 0, may hold values from -6 to 6
- out_weight: bfloat16 [8192, 4096], P(('shift', 'dp')), parts along dimension 0, may hold values from -0.09375 to 0.09375
Outputs:
- mixer_out: bfloat16 [8, 1024, 4096], P(('shift', 'dp'), 'sp'), parts along dimension 0
The draws below stay inside these ranges and needn't reach their ends.
There are 2 independent parts, one for each index of `shift`. The reference program is written for one: setup_inputs(seed, part) draws one part's arguments, and reference() takes and returns one part's arrays. A program takes and returns all parts, laid end to end along the dimension named above; each array names one. Nothing has to cross between parts.
All inputs are finite; a program needn't handle non-finite values.
Results may differ from the reference program's by a relative error of at most 0.006.
Values may be sent and summed in bfloat16 or wider, within the bound.
A program may use at most 128 MiB of HBM per device.

```python
import jax
import jax.numpy as jnp
from jax import lax

HEADS = 32
HEAD_SIZE = 128
BATCH = 4
TOKENS = 1024
WIDTH = 4096


def steps_of(key, shape, shards, least, top_value):
    factor_of = 1.0
    for dim, shards_of in shards:
        steps = jax.random.uniform(jax.random.fold_in(jax.random.fold_in(key, 6), dim), (shards_of,), jnp.float32, least / len(shards), top_value / len(shards))
        factor_of = factor_of * jnp.repeat(jnp.exp(steps), shape[dim] // shards_of).reshape((-1,) + (1,) * (len(shape) - 1 - dim))
    return factor_of


def noise(key, dims, scale, most, cuts=(), dtype=jnp.bfloat16):
    entries = jax.random.normal(key, dims, jnp.float32) * scale
    if len(cuts) > 0:
        entries = steps_of(key, dims, cuts, -0.22, 0.18) * entries
    return jnp.clip(entries, min=-most, max=most).astype(dtype)


def setup_inputs(seed: int = 0, part: int = 0) -> dict:
    key_of = jax.random.split(jax.random.key(seed), 5)
    own_keys = jax.random.split(jax.random.fold_in(key_of[4], part), 5)
    return {
        "query_rows": noise(own_keys[0], (BATCH, TOKENS, HEADS, HEAD_SIZE), 1.0, 6.0, ((0, 4), (1, 4))),
        "key_rows": noise(own_keys[1], (BATCH, TOKENS, HEADS, HEAD_SIZE), 1.0, 6.0, ((0, 4), (1, 4))),
        "value_rows": noise(own_keys[2], (BATCH, TOKENS, HEADS, HEAD_SIZE), 1.0, 6.0, ((0, 4), (1, 4))),
        "out_weight": noise(own_keys[3], (WIDTH, WIDTH), WIDTH ** -0.5, 0.09375, ((0, 4),)),
    }


def feature_map(values):
    wide = values.astype(jnp.float32)
    return (jnp.where(wide > 0.0, wide + 1.0, jnp.exp(jnp.minimum(wide, 0.0)))).astype(jnp.bfloat16)


def finish_heads(read, count):
    result = read * count ** 0.5
    return result.astype(jnp.bfloat16)


def ask_state(features, state, mass):
    small = lax.optimization_barrier(state.astype(jnp.bfloat16))
    top = jnp.einsum("bthd,bhde->bthe", features.astype(jnp.float32), small.astype(jnp.float32))
    bottom = jnp.einsum("bthd,bhd->bth", features.astype(jnp.float32), mass, precision=lax.Precision.HIGHEST)
    return top / (bottom + 1e-3)[..., None]


def reference(query_rows, key_rows, value_rows, out_weight):
    query_feature, key_feature = lax.optimization_barrier((feature_map(query_rows), feature_map(key_rows)))
    state = jnp.einsum("bthd,bthe->bhde", key_feature.astype(jnp.float32), value_rows.astype(jnp.float32)) / TOKENS
    mass = jnp.sum(key_feature.astype(jnp.float32), axis=1) / TOKENS
    mixed = finish_heads(ask_state(query_feature, state, mass), TOKENS).reshape(BATCH, TOKENS, WIDTH)
    mixed = lax.optimization_barrier(mixed)
    mixer_out = jnp.einsum("btw,wv->btv", mixed.astype(jnp.float32), out_weight.astype(jnp.float32)).astype(jnp.bfloat16)
    return mixer_out
```

```python
import jax
import jax.numpy as jnp
from jax import lax
from jax.sharding import PartitionSpec as P


def feature_map(values):
    wide = values.astype(jnp.float32)
    return jnp.where(wide > 0.0, wide + 1.0, jnp.exp(jnp.minimum(wide, 0.0))).astype(jnp.bfloat16)


def plain_body(query_rows, key_rows, value_rows, out_weight):
    query_feature, key_feature = (feature_map(query_rows), feature_map(key_rows))
    count = query_rows.shape[1] * lax.axis_size("sp")
    state = (
        jnp.einsum("bthd,bthe->bhde", key_feature, value_rows, preferred_element_type=jnp.float32)
        / count
    )
    mass = jnp.sum(key_feature.astype(jnp.float32), axis=1) / count
    state = lax.psum(state.astype(jnp.bfloat16), "sp")
    mass = lax.psum(mass, "sp")
    top = jnp.einsum("bthd,bhde->bthe", query_feature, state, preferred_element_type=jnp.float32)
    bottom = jnp.einsum(
        "bthd,bhd->bth", query_feature.astype(jnp.float32), mass, precision=lax.Precision.HIGHEST
    )
    mixed = (top / (bottom + 0.001)[..., None] * count**0.5).astype(jnp.bfloat16)
    mixed = mixed.reshape(mixed.shape[0], mixed.shape[1], -1)
    mine = lax.all_to_all(mixed, "dp", split_axis=2, concat_axis=0, tiled=True)
    part = jnp.einsum("btw,wv->btv", mine, out_weight, preferred_element_type=jnp.float32)
    return lax.psum_scatter(part.astype(jnp.bfloat16), "dp", scatter_dimension=0, tiled=True)


def solution(mesh):
    placed = (
        P(("shift", "dp"), "sp", None, None),
        P(("shift", "dp"), "sp", None, None),
        P(("shift", "dp"), "sp", None, None),
        P(("shift", "dp"), None),
    )
    return jax.shard_map(
        plain_body, mesh=mesh, in_specs=placed, out_specs=P(("shift", "dp"), "sp", None), check_vma=False
    )
```

```python
import functools

import jax
import jax.numpy as jnp
from jax import lax
from jax.experimental import pallas as pl
from jax.experimental.pallas import tpu as pltpu
from jax.sharding import PartitionSpec as P


def feature_map(values):
    wide = values.astype(jnp.float32)
    return jnp.where(wide > 0.0, wide + 1.0, jnp.exp(jnp.minimum(wide, 0.0))).astype(jnp.bfloat16)


def plain_body(query_rows, key_rows, value_rows, out_weight):
    query_feature, key_feature = (feature_map(query_rows), feature_map(key_rows))
    count = query_rows.shape[1] * lax.axis_size("sp")
    state = (
        jnp.einsum("bthd,bthe->bhde", key_feature, value_rows, preferred_element_type=jnp.float32)
        / count
    )
    mass = jnp.sum(key_feature.astype(jnp.float32), axis=1) / count
    state = lax.psum(state.astype(jnp.bfloat16), "sp")
    mass = lax.psum(mass, "sp")
    top = jnp.einsum("bthd,bhde->bthe", query_feature, state, preferred_element_type=jnp.float32)
    bottom = jnp.einsum(
        "bthd,bhd->bth", query_feature.astype(jnp.float32), mass, precision=lax.Precision.HIGHEST
    )
    mixed = (top / (bottom + 0.001)[..., None] * count**0.5).astype(jnp.bfloat16)
    mixed = mixed.reshape(mixed.shape[0], mixed.shape[1], -1)
    mine = lax.all_to_all(mixed, "dp", split_axis=2, concat_axis=0, tiled=True)
    part = jnp.einsum("btw,wv->btv", mine, out_weight, preferred_element_type=jnp.float32)
    return lax.psum_scatter(part.astype(jnp.bfloat16), "dp", scatter_dimension=0, tiled=True)


MESH = pl.DeviceIdType.MESH
EXTRA = 16
NT = (((1,), (1,)), ((), ()))


def remote(src, dst, send, recv, **where):
    return pltpu.make_async_remote_copy(
        src_ref=src, dst_ref=dst, send_sem=send, recv_sem=recv, device_id=where, device_id_type=MESH
    )


def kernel(
    ND, NS, A, B, count, q_ref, st_ref, w_hbm, out_ref,
    w, qall, st1, red, stall, mixed, part, r1e, r1o, s2e, s2o, keep, r2e, r2o,
    wsem, lsem, qs, qr, ss1, rs1, ss2, rs2, e1s, e1r, o1s, o1r, e2s, e2r, o2s, o2r,
):
    d, p = lax.axis_index("dp"), lax.axis_index("sp")
    i, j = lax.div(d, B), lax.rem(d, B)
    HD, HS, size = q_ref.shape[1], st_ref.shape[2], q_ref.shape[3]
    half, C = part.shape[0] // 2, part.shape[-1]

    def at(base, r, n):
        return lax.rem(base + r + n, n)

    barrier = pltpu.get_barrier_semaphore()
    for rd in range(ND):
        for rp in range(NS):
            if rd or rp:
                pl.semaphore_signal(
                    barrier, inc=1, device_id={"dp": at(d, rd, ND), "sp": at(p, rp, NS)}, device_id_type=MESH
                )
    pl.semaphore_wait(barrier, ND * NS - 1)

    first = []
    for r in range(1, NS):
        pp = at(p, r, NS)
        copy = remote(st_ref.at[:, pp], st1.at[r - 1], ss1.at[r], rs1.at[r], sp=pp)
        copy.start()
        first.append(copy)
    queries = {}
    for r in range(1, ND):
        dd = at(d, r, ND)
        queries[r] = remote(q_ref.at[dd], qall.at[d], qs.at[r], qr.at[r], dp=dd)
        queries[r].start()
    own_query = pltpu.make_async_copy(q_ref.at[d], qall.at[d], lsem.at[0])
    own_query.start()
    weights = pltpu.make_async_copy(w_hbm, w, wsem)
    weights.start()

    for copy in first:
        copy.wait()

    @pl.loop(0, ND)
    def _(x):
        total = st_ref[x, p].astype(jnp.float32)
        for r in range(1, NS):
            total += st1[r - 1, x].astype(jnp.float32)
        red[x] = total.astype(red.dtype)

    second = {}
    for rp in range(NS - 1, -1, -1):
        for rd in range(ND):
            if rd or rp:
                dd, pp = at(d, rd, ND), at(p, rp, NS)
                second[rd, rp] = remote(
                    red.at[dd], stall.at[d, p], ss2.at[rd, rp], rs2.at[rd, rp], dp=dd, sp=pp
                )
                second[rd, rp].start()
    own_state = pltpu.make_async_copy(red.at[d], stall.at[d, p], lsem.at[1])
    own_state.start()

    for rd in range(ND):
        s = at(d, -rd, ND)
        if rd:
            remote(q_ref.at[d], qall.at[s], qs.at[rd], qr.at[rd], dp=s).wait_recv()
        else:
            own_query.wait()
            own_state.wait()
        for rp in range(NS):
            if rd or rp:
                pp = at(p, -rp, NS)
                remote(red.at[d], stall.at[s, pp], ss2.at[rd, rp], rs2.at[rd, rp], dp=s, sp=pp).wait_recv()

        @pl.loop(0, NS)
        def _(pp):
            for k in range(HS):
                head = pp * HS + k
                both = stall[s, pp, k]
                both = jnp.concatenate([both[:size]] + [both[size:]] * (size // EXTRA), axis=0)
                read = lax.dot_general(qall[s, head], both, NT, preferred_element_type=jnp.float32)
                read = read[:, :size] / (read[:, size:] + 0.001) * count**0.5
                mixed[s, :, pl.ds(pl.multiple_of(head * size, size), size)] = read.astype(mixed.dtype)

    weights.wait()

    def e1(c, r):
        jj = at(j, r, B)
        return remote(part.at[2 * c, :, jj], r1e.at[c, r - 1], e1s.at[c, r], e1r.at[c, r], dp=i * B + jj)

    def o1(c, r):
        ii = at(i, r, A)
        return remote(part.at[2 * c + 1, ii], r1o.at[c, r - 1], o1s.at[c, r], o1r.at[c, r], dp=ii * B + j)

    def e2(c, r):
        ii = at(i, r, A)
        return remote(s2e.at[c, ii], r2e.at[c, r - 1], e2s.at[c, r], e2r.at[c, r], dp=ii * B + j)

    def o2(c, r):
        jj = at(j, r, B)
        return remote(s2o.at[c, jj], r2o.at[c, r - 1], o2s.at[c, r], o2r.at[c, r], dp=i * B + jj)

    @pl.loop(0, half)
    def _(c):
        for odd in range(2):
            columns = pl.ds(pl.multiple_of((2 * c + odd) * C, C), C)

            @pl.loop(0, ND)
            def _(s):
                block = jnp.dot(mixed[s], w[:, columns], preferred_element_type=jnp.float32)
                part[2 * c + odd, lax.div(s, B), lax.rem(s, B)] = block.astype(part.dtype)

            for r in range(1, A if odd else B):
                (o1 if odd else e1)(c, r).start()

    @pl.loop(0, half)
    def _(c):
        for r in range(1, B):
            e1(c, r).wait_recv()
        for r in range(A):
            ii = at(i, r, A)
            total = part[2 * c, ii, j].astype(jnp.float32)
            for k in range(1, B):
                total += r1e[c, k - 1, ii].astype(jnp.float32)
            if r:
                s2e[c, ii] = total.astype(s2e.dtype)
                e2(c, r).start()
            else:
                keep[2 * c] = total
        for r in range(1, A):
            o1(c, r).wait_recv()
        for r in range(B):
            jj = at(j, r, B)
            total = part[2 * c + 1, i, jj].astype(jnp.float32)
            for k in range(1, A):
                total += r1o[c, k - 1, jj].astype(jnp.float32)
            if r:
                s2o[c, jj] = total.astype(s2o.dtype)
                o2(c, r).start()
            else:
                keep[2 * c + 1] = total

    @pl.loop(0, half)
    def _(c):
        for odd, n, copies, slots in ((0, A, e2, r2e), (1, B, o2, r2o)):
            total = keep[2 * c + odd]
            for r in range(1, n):
                copies(c, r).wait_recv()
                total += slots[c, r - 1].astype(jnp.float32)
            columns = pl.ds(pl.multiple_of((2 * c + odd) * C, C), C)
            out_ref[:, columns] = total.astype(out_ref.dtype)

    for r in range(1, ND):
        queries[r].wait_send()
    for copy in second.values():
        copy.wait_send()

    @pl.loop(0, half)
    def _(c):
        for r in range(1, B):
            e1(c, r).wait_send()
            o2(c, r).wait_send()
        for r in range(1, A):
            o1(c, r).wait_send()
            e2(c, r).wait_send()


def split_of(n):
    for a in range(int(n**0.5), 0, -1):
        if n % a == 0:
            return a, n // a


def kernel_body(query_rows, key_rows, value_rows, out_weight):
    ND, NS = lax.axis_size("dp"), lax.axis_size("sp")
    _, T, H, size = query_rows.shape
    V, rows = out_weight.shape[1], out_weight.shape[0]
    A, B = split_of(ND)
    HD, HS, NC = H // ND, H // ND // NS, 8
    C, half, count = V // NC, NC // 2, T * NS
    key_feature = feature_map(key_rows)
    state = jnp.einsum(
        "bthd,bthe->bhed", key_feature, value_rows, preferred_element_type=jnp.float32
    )[0] / count
    mass = jnp.sum(key_feature.astype(jnp.float32), axis=1)[0] / count
    mass = jnp.broadcast_to(mass[:, None, :].astype(jnp.bfloat16), (H, EXTRA, size))
    state = jnp.concatenate([state.astype(jnp.bfloat16), mass], axis=1).reshape(ND, NS, HS, size + EXTRA, size)
    query = feature_map(query_rows)[0].transpose(1, 0, 2).reshape(ND, HD, T, size)
    bf, block = jnp.bfloat16, (HS, size + EXTRA, size)
    dma = pltpu.SemaphoreType.DMA
    out = pl.pallas_call(
        functools.partial(kernel, ND, NS, A, B, count),
        out_shape=jax.ShapeDtypeStruct((T, V), bf),
        in_specs=[
            pl.BlockSpec(memory_space=pltpu.VMEM),
            pl.BlockSpec(memory_space=pltpu.VMEM),
            pl.BlockSpec(memory_space=pl.ANY),
        ],
        out_specs=pl.BlockSpec(memory_space=pltpu.VMEM),
        scratch_shapes=[
            pltpu.VMEM((rows, V), bf),
            pltpu.VMEM((ND, HD, T, size), bf),
            pltpu.VMEM((NS - 1, ND) + block, bf),
            pltpu.VMEM((ND,) + block, bf),
            pltpu.VMEM((ND, NS) + block, bf),
            pltpu.VMEM((ND, T, HD * size), bf),
            pltpu.VMEM((NC, A, B, T, C), bf),
            pltpu.VMEM((half, B - 1, A, T, C), bf),
            pltpu.VMEM((half, A - 1, B, T, C), bf),
            pltpu.VMEM((half, A, T, C), bf),
            pltpu.VMEM((half, B, T, C), bf),
            pltpu.VMEM((NC, T, C), jnp.float32),
            pltpu.VMEM((half, A - 1, T, C), bf),
            pltpu.VMEM((half, B - 1, T, C), bf),
            dma, dma((2,)), dma((ND,)), dma((ND,)), dma((NS,)), dma((NS,)), dma((ND, NS)), dma((ND, NS)),
            dma((half, B)), dma((half, B)), dma((half, A)), dma((half, A)),
            dma((half, A)), dma((half, A)), dma((half, B)), dma((half, B)),
        ],
        compiler_params=pltpu.CompilerParams(
            collective_id=0, has_side_effects=True, vmem_limit_bytes=63 * 2**20
        ),
    )(query, state, out_weight)
    return out[None]


def body(query_rows, key_rows, value_rows, out_weight):
    ND, NS = lax.axis_size("dp"), lax.axis_size("sp")
    batch, T, H, size = query_rows.shape
    rows, V = out_weight.shape
    need = 2 * rows * V + 2 * ND * T * V * 2 + 2 * T * V * 8 + 4 * H * T * size * 2
    fits = batch == 1 and H % (ND * NS) == 0 and V % 1024 == 0 and min(split_of(ND)) > 1
    fits = fits and size == 128 and T % 16 == 0 and need < 56 * 2**20
    run = kernel_body if fits else plain_body
    return run(query_rows, key_rows, value_rows, out_weight)


def solution(mesh):
    placed = (
        P(("shift", "dp"), "sp", None, None),
        P(("shift", "dp"), "sp", None, None),
        P(("shift", "dp"), "sp", None, None),
        P(("shift", "dp"), None),
    )
    return jax.shard_map(
        body, mesh=mesh, in_specs=placed, out_specs=P(("shift", "dp"), "sp", None), check_vma=False
    )
```

```python
import functools

import jax
import jax.numpy as jnp
from jax import lax
from jax.experimental import pallas as pl
from jax.experimental.pallas import tpu as pltpu
from jax.sharding import PartitionSpec as P


def feature_map(values):
    wide = values.astype(jnp.float32)
    return jnp.where(wide > 0.0, wide + 1.0, jnp.exp(jnp.minimum(wide, 0.0))).astype(jnp.bfloat16)


def plain_body(query_rows, key_rows, value_rows, out_weight):
    query_feature, key_feature = (feature_map(query_rows), feature_map(key_rows))
    count = query_rows.shape[1] * lax.axis_size("sp")
    state = (
        jnp.einsum("bthd,bthe->bhde", key_feature, value_rows, preferred_element_type=jnp.float32)
        / count
    )
    mass = jnp.sum(key_feature.astype(jnp.float32), axis=1) / count
    state = lax.psum(state.astype(jnp.bfloat16), "sp")
    mass = lax.psum(mass, "sp")
    top = jnp.einsum("bthd,bhde->bthe", query_feature, state, preferred_element_type=jnp.float32)
    bottom = jnp.einsum(
        "bthd,bhd->bth", query_feature.astype(jnp.float32), mass, precision=lax.Precision.HIGHEST
    )
    mixed = (top / (bottom + 0.001)[..., None] * count**0.5).astype(jnp.bfloat16)
    mixed = mixed.reshape(mixed.shape[0], mixed.shape[1], -1)
    mine = lax.all_to_all(mixed, "dp", split_axis=2, concat_axis=0, tiled=True)
    part = jnp.einsum("btw,wv->btv", mine, out_weight, preferred_element_type=jnp.float32)
    return lax.psum_scatter(part.astype(jnp.bfloat16), "dp", scatter_dimension=0, tiled=True)


MESH = pl.DeviceIdType.MESH
EXTRA = 16
NT = (((1,), (1,)), ((), ()))


def remote(src, dst, send, recv, **where):
    return pltpu.make_async_remote_copy(
        src_ref=src, dst_ref=dst, send_sem=send, recv_sem=recv, device_id=where, device_id_type=MESH
    )


def kernel(
    ND, NS, A, B, count, q_hbm, st_ref, w_hbm, out_ref,
    qraw, qwide, q_ref, w, qall, st1, red, stall, mixed, part, r1e, r1o, s2e, s2o, keep, r2e, r2o,
    wsem, qsem, lsem, qs, qr, ss1, rs1, ss2, rs2, e1s, e1r, o1s, o1r, e2s, e2r, o2s, o2r,
):
    d, p = lax.axis_index("dp"), lax.axis_index("sp")
    i, j = lax.div(d, B), lax.rem(d, B)
    HD, HS, size = q_ref.shape[1], st_ref.shape[2], q_ref.shape[3]
    half, C = part.shape[0] // 2, part.shape[-1]

    def at(base, r, n):
        return lax.rem(base + r + n, n)

    def twin(r):
        other, bit = p, 1
        while bit <= r:
            if r & bit:
                other = other + bit - 2 * bit * lax.rem(lax.div(p, bit), 2)
            bit *= 2
        return other

    load = pltpu.make_async_copy(q_hbm, qraw, qsem)
    load.start()
    weights = pltpu.make_async_copy(w_hbm, w, wsem)
    weights.start()

    barrier = pltpu.get_barrier_semaphore()
    for rd in range(ND):
        for rp in range(NS):
            if rd or rp:
                pl.semaphore_signal(
                    barrier, inc=1, device_id={"dp": at(d, rd, ND), "sp": at(p, rp, NS)}, device_id_type=MESH
                )
    pl.semaphore_wait(barrier, ND * NS - 1)

    order = list(range(NS - 1, 0, -1))
    first = {}
    for rd in range(ND):
        dd = at(d, rd, ND)
        for r in order:
            pp = twin(r)
            first[rd, r] = remote(
                st_ref.at[dd, pp], st1.at[r - 1, dd], ss1.at[rd, r], rs1.at[rd, r], sp=pp
            )
            first[rd, r].start()

    load.wait()
    tokens, heads, step = q_ref.shape[2], ND * HD, 1024

    @pl.loop(0, tokens * heads // step)
    def _(x):
        rows = pl.ds(pl.multiple_of(x * step, step), step)
        wide = qraw[rows].astype(jnp.float32)
        qwide[rows] = jnp.where(wide > 0.0, wide + 1.0, jnp.exp(jnp.minimum(wide, 0.0)))

    @pl.loop(0, ND)
    def _(x):
        for k in range(HD):
            q_ref[x, k] = qwide[pl.ds(x * HD + k, tokens, stride=heads), :].astype(q_ref.dtype)

    queries = {}
    for r in range(1, ND):
        dd = at(d, r, ND)
        queries[r] = remote(q_ref.at[dd], qall.at[d], qs.at[r], qr.at[r], dp=dd)
        queries[r].start()
    own_query = pltpu.make_async_copy(q_ref.at[d], qall.at[d], lsem.at[0])
    own_query.start()

    second = {}
    for rd in range(ND):
        dd = at(d, rd, ND)
        total = st_ref[dd, p].astype(jnp.float32)
        for r in order:
            first[rd, r].wait_recv()
            total += st1[r - 1, dd].astype(jnp.float32)
        red[dd] = total.astype(red.dtype)
        for rp in [0] + order:
            if rd or rp:
                second[rd, rp] = remote(
                    red.at[dd], stall.at[d, p], ss2.at[rd, rp], rs2.at[rd, rp], dp=dd, sp=twin(rp)
                )
                second[rd, rp].start()
            else:
                own_state = pltpu.make_async_copy(red.at[d], stall.at[d, p], lsem.at[1])
                own_state.start()

    for rp in [0] + order:
        pp = twin(rp)
        for rd in range(ND):
            s = at(d, -rd, ND)
            if rp == 0 and rd:
                remote(q_ref.at[d], qall.at[s], qs.at[rd], qr.at[rd], dp=s).wait_recv()
            if rd or rp:
                remote(red.at[d], stall.at[s, pp], ss2.at[rd, rp], rs2.at[rd, rp], dp=s, sp=pp).wait_recv()
            else:
                own_query.wait()
                own_state.wait()

        @pl.loop(0, ND)
        def _(s):
            for k in range(HS):
                head = pp * HS + k
                both = stall[s, pp, k]
                both = jnp.concatenate([both[:size]] + [both[size:]] * (size // EXTRA), axis=0)
                read = lax.dot_general(qall[s, head], both, NT, preferred_element_type=jnp.float32)
                read = read[:, :size] / (read[:, size:] + 0.001) * count**0.5
                mixed[s, :, pl.ds(pl.multiple_of(head * size, size), size)] = read.astype(mixed.dtype)

    weights.wait()

    def e1(c, r):
        jj = at(j, r, B)
        return remote(part.at[2 * c, :, jj], r1e.at[c, r - 1], e1s.at[c, r], e1r.at[c, r], dp=i * B + jj)

    def o1(c, r):
        ii = at(i, r, A)
        return remote(part.at[2 * c + 1, ii], r1o.at[c, r - 1], o1s.at[c, r], o1r.at[c, r], dp=ii * B + j)

    def e2(c, r):
        ii = at(i, r, A)
        return remote(s2e.at[c, ii], r2e.at[c, r - 1], e2s.at[c, r], e2r.at[c, r], dp=ii * B + j)

    def o2(c, r):
        jj = at(j, r, B)
        return remote(s2o.at[c, jj], r2o.at[c, r - 1], o2s.at[c, r], o2r.at[c, r], dp=i * B + jj)

    @pl.loop(0, half)
    def _(c):
        for odd in range(2):
            columns = pl.ds(pl.multiple_of((2 * c + odd) * C, C), C)

            @pl.loop(0, ND)
            def _(s):
                block = jnp.dot(mixed[s], w[:, columns], preferred_element_type=jnp.float32)
                part[2 * c + odd, lax.div(s, B), lax.rem(s, B)] = block.astype(part.dtype)

            for r in range(1, A if odd else B):
                (o1 if odd else e1)(c, r).start()

    @pl.loop(0, half)
    def _(c):
        for r in range(1, B):
            e1(c, r).wait_recv()
        for r in range(A):
            ii = at(i, r, A)
            total = part[2 * c, ii, j].astype(jnp.float32)
            for k in range(1, B):
                total += r1e[c, k - 1, ii].astype(jnp.float32)
            if r:
                s2e[c, ii] = total.astype(s2e.dtype)
                e2(c, r).start()
            else:
                keep[2 * c] = total
        for r in range(1, A):
            o1(c, r).wait_recv()
        for r in range(B):
            jj = at(j, r, B)
            total = part[2 * c + 1, i, jj].astype(jnp.float32)
            for k in range(1, A):
                total += r1o[c, k - 1, jj].astype(jnp.float32)
            if r:
                s2o[c, jj] = total.astype(s2o.dtype)
                o2(c, r).start()
            else:
                keep[2 * c + 1] = total

    @pl.loop(0, half)
    def _(c):
        for odd, n, copies, slots in ((0, A, e2, r2e), (1, B, o2, r2o)):
            total = keep[2 * c + odd]
            for r in range(1, n):
                copies(c, r).wait_recv()
                total += slots[c, r - 1].astype(jnp.float32)
            columns = pl.ds(pl.multiple_of((2 * c + odd) * C, C), C)
            out_ref[:, columns] = total.astype(out_ref.dtype)

    for r in range(1, ND):
        queries[r].wait_send()
    for copy in list(first.values()) + list(second.values()):
        copy.wait_send()

    @pl.loop(0, half)
    def _(c):
        for r in range(1, B):
            e1(c, r).wait_send()
            o2(c, r).wait_send()
        for r in range(1, A):
            o1(c, r).wait_send()
            e2(c, r).wait_send()


def split_of(n):
    for a in range(int(n**0.5), 0, -1):
        if n % a == 0:
            return a, n // a


def kernel_body(query_rows, key_rows, value_rows, out_weight):
    ND, NS = lax.axis_size("dp"), lax.axis_size("sp")
    _, T, H, size = query_rows.shape
    V, rows = out_weight.shape[1], out_weight.shape[0]
    A, B = split_of(ND)
    HD, HS, NC = H // ND, H // ND // NS, 8
    C, half, count = V // NC, NC // 2, T * NS
    key_feature = feature_map(key_rows)
    state = jnp.einsum(
        "bthd,bthe->bhed", key_feature, value_rows, preferred_element_type=jnp.float32
    )[0] / count
    mass = jnp.sum(key_feature.astype(jnp.float32), axis=1)[0] / count
    mass = jnp.broadcast_to(mass[:, None, :].astype(jnp.bfloat16), (H, EXTRA, size))
    state = jnp.concatenate([state.astype(jnp.bfloat16), mass], axis=1).reshape(ND, NS, HS, size + EXTRA, size)
    query = query_rows.reshape(T * H, size)
    bf, block = jnp.bfloat16, (HS, size + EXTRA, size)
    dma = pltpu.SemaphoreType.DMA
    out = pl.pallas_call(
        functools.partial(kernel, ND, NS, A, B, count),
        out_shape=jax.ShapeDtypeStruct((T, V), bf),
        in_specs=[
            pl.BlockSpec(memory_space=pl.ANY),
            pl.BlockSpec(memory_space=pltpu.VMEM),
            pl.BlockSpec(memory_space=pl.ANY),
        ],
        out_specs=pl.BlockSpec(memory_space=pltpu.VMEM),
        scratch_shapes=[
            pltpu.VMEM((T * H, size), bf),
            pltpu.VMEM((T * H, size), jnp.float32),
            pltpu.VMEM((ND, HD, T, size), bf),
            pltpu.VMEM((rows, V), bf),
            pltpu.VMEM((ND, HD, T, size), bf),
            pltpu.VMEM((NS - 1, ND) + block, bf),
            pltpu.VMEM((ND,) + block, bf),
            pltpu.VMEM((ND, NS) + block, bf),
            pltpu.VMEM((ND, T, HD * size), bf),
            pltpu.VMEM((NC, A, B, T, C), bf),
            pltpu.VMEM((half, B - 1, A, T, C), bf),
            pltpu.VMEM((half, A - 1, B, T, C), bf),
            pltpu.VMEM((half, A, T, C), bf),
            pltpu.VMEM((half, B, T, C), bf),
            pltpu.VMEM((NC, T, C), jnp.float32),
            pltpu.VMEM((half, A - 1, T, C), bf),
            pltpu.VMEM((half, B - 1, T, C), bf),
            dma, dma, dma((2,)), dma((ND,)), dma((ND,)), dma((ND, NS)), dma((ND, NS)), dma((ND, NS)), dma((ND, NS)),
            dma((half, B)), dma((half, B)), dma((half, A)), dma((half, A)),
            dma((half, A)), dma((half, A)), dma((half, B)), dma((half, B)),
        ],
        compiler_params=pltpu.CompilerParams(
            collective_id=0, has_side_effects=True, vmem_limit_bytes=63 * 2**20
        ),
    )(query, state, out_weight)
    return out[None]


def body(query_rows, key_rows, value_rows, out_weight):
    ND, NS = lax.axis_size("dp"), lax.axis_size("sp")
    batch, T, H, size = query_rows.shape
    rows, V = out_weight.shape
    need = 2 * rows * V + 2 * ND * T * V * 2 + 2 * T * V * 8 + 6 * H * T * size * 2
    fits = batch == 1 and H % (ND * NS) == 0 and V % 1024 == 0 and min(split_of(ND)) > 1
    fits = fits and size == 128 and T % 16 == 0 and T * H % 1024 == 0 and NS & (NS - 1) == 0 and need < 56 * 2**20
    run = kernel_body if fits else plain_body
    return run(query_rows, key_rows, value_rows, out_weight)


def solution(mesh):
    placed = (
        P(("shift", "dp"), "sp", None, None),
        P(("shift", "dp"), "sp", None, None),
        P(("shift", "dp"), "sp", None, None),
        P(("shift", "dp"), None),
    )
    return jax.shard_map(
        body, mesh=mesh, in_specs=placed, out_specs=P(("shift", "dp"), "sp", None), check_vma=False
    )
```

```python
import functools

import jax
import jax.numpy as jnp
from jax import lax
from jax.experimental import pallas as pl
from jax.experimental.pallas import tpu as pltpu
from jax.sharding import PartitionSpec as P


def feature_map(values):
    wide = values.astype(jnp.float32)
    return jnp.where(wide > 0.0, wide + 1.0, jnp.exp(jnp.minimum(wide, 0.0))).astype(jnp.bfloat16)


def plain_body(query_rows, key_rows, value_rows, out_weight):
    query_feature, key_feature = (feature_map(query_rows), feature_map(key_rows))
    count = query_rows.shape[1] * lax.axis_size("sp")
    state = (
        jnp.einsum("bthd,bthe->bhde", key_feature, value_rows, preferred_element_type=jnp.float32)
        / count
    )
    mass = jnp.sum(key_feature.astype(jnp.float32), axis=1) / count
    state = lax.psum(state.astype(jnp.bfloat16), "sp")
    mass = lax.psum(mass, "sp")
    top = jnp.einsum("bthd,bhde->bthe", query_feature, state, preferred_element_type=jnp.float32)
    bottom = jnp.einsum(
        "bthd,bhd->bth", query_feature.astype(jnp.float32), mass, precision=lax.Precision.HIGHEST
    )
    mixed = (top / (bottom + 0.001)[..., None] * count**0.5).astype(jnp.bfloat16)
    mixed = mixed.reshape(mixed.shape[0], mixed.shape[1], -1)
    mine = lax.all_to_all(mixed, "dp", split_axis=2, concat_axis=0, tiled=True)
    part = jnp.einsum("btw,wv->btv", mine, out_weight, preferred_element_type=jnp.float32)
    return lax.psum_scatter(part.astype(jnp.bfloat16), "dp", scatter_dimension=0, tiled=True)


MESH = pl.DeviceIdType.MESH
EXTRA = 16
NT = (((1,), (1,)), ((), ()))


def remote(src, dst, send, recv, **where):
    return pltpu.make_async_remote_copy(
        src_ref=src, dst_ref=dst, send_sem=send, recv_sem=recv, device_id=where, device_id_type=MESH
    )


def kernel(
    ND, NS, A, B, count, q_hbm, st_ref, w_hbm, out_ref,
    qraw, qwide, q_ref, w, qall, st1, red, stall, mixed, part, r1e, r1o, s2e, s2o, keep, r2e, r2o,
    wsem, qsem, lsem, qs, qr, ss1, rs1, ss2, rs2, e1s, e1r, o1s, o1r, e2s, e2r, o2s, o2r,
):
    d, p = lax.axis_index("dp"), lax.axis_index("sp")
    i, j = lax.div(d, B), lax.rem(d, B)
    HD, HS, size = q_ref.shape[1], st_ref.shape[2], q_ref.shape[3]
    half, C = part.shape[0] // 2, part.shape[-1]

    def at(base, r, n):
        return lax.rem(base + r + n, n)

    def twin(r):
        other, bit = p, 1
        while bit <= r:
            if r & bit:
                other = other + bit - 2 * bit * lax.rem(lax.div(p, bit), 2)
            bit *= 2
        return other

    load = pltpu.make_async_copy(q_hbm, qraw, qsem)
    load.start()
    weights = pltpu.make_async_copy(w_hbm, w, wsem)
    weights.start()

    barrier = pltpu.get_barrier_semaphore()
    for rd in range(ND):
        for rp in range(NS):
            if rd or rp:
                pl.semaphore_signal(
                    barrier, inc=1, device_id={"dp": at(d, rd, ND), "sp": at(p, rp, NS)}, device_id_type=MESH
                )
    pl.semaphore_wait(barrier, ND * NS - 1)

    order = list(range(NS - 1, 0, -1))
    first = {}
    for rd in range(ND):
        dd = at(d, rd, ND)
        for r in order:
            pp = twin(r)
            first[rd, r] = remote(
                st_ref.at[dd, pp], st1.at[r - 1, dd], ss1.at[rd, r], rs1.at[rd, r], sp=pp
            )
            first[rd, r].start()

    load.wait()
    tokens, heads, step = q_ref.shape[2], ND * HD, 1024

    @pl.loop(0, tokens * heads // step)
    def _(x):
        rows = pl.ds(pl.multiple_of(x * step, step), step)
        wide = qraw[rows].astype(jnp.float32)
        qwide[rows] = jnp.where(wide > 0.0, wide + 1.0, jnp.exp(jnp.minimum(wide, 0.0)))

    @pl.loop(0, ND)
    def _(x):
        for k in range(HD):
            q_ref[x, k] = qwide[pl.ds(x * HD + k, tokens, stride=heads), :].astype(q_ref.dtype)

    queries = {}
    for r in range(1, ND):
        dd = at(d, r, ND)
        queries[r] = remote(q_ref.at[dd], qall.at[d], qs.at[r], qr.at[r], dp=dd)
        queries[r].start()
    own_query = pltpu.make_async_copy(q_ref.at[d], qall.at[d], lsem.at[0])
    own_query.start()

    second = {}
    for rd in range(ND):
        dd = at(d, rd, ND)
        total = st_ref[dd, p].astype(jnp.float32)
        for r in order:
            first[rd, r].wait_recv()
            total += st1[r - 1, dd].astype(jnp.float32)
        red[dd] = total.astype(red.dtype)
        for rp in [0] + order:
            if rd or rp:
                second[rd, rp] = remote(
                    red.at[dd], stall.at[d, p], ss2.at[rd, rp], rs2.at[rd, rp], dp=dd, sp=twin(rp)
                )
                second[rd, rp].start()
            else:
                own_state = pltpu.make_async_copy(red.at[d], stall.at[d, p], lsem.at[1])
                own_state.start()

    for rp in [0] + order:
        pp = twin(rp)
        for rd in range(ND):
            s = at(d, -rd, ND)
            if rp == 0 and rd:
                remote(q_ref.at[d], qall.at[s], qs.at[rd], qr.at[rd], dp=s).wait_recv()
            if rd or rp:
                remote(red.at[d], stall.at[s, pp], ss2.at[rd, rp], rs2.at[rd, rp], dp=s, sp=pp).wait_recv()
            else:
                own_query.wait()
                own_state.wait()

        @pl.loop(0, ND)
        def _(s):
            for k in range(HS):
                head = pp * HS + k
                both = stall[s, pp, k]
                both = jnp.concatenate([both[:size]] + [both[size:]] * (size // EXTRA), axis=0)
                read = lax.dot_general(qall[s, head], both, NT, preferred_element_type=jnp.float32)
                read = read[:, :size] / (read[:, size:] + 0.001) * count**0.5
                mixed[s, :, pl.ds(pl.multiple_of(head * size, size), size)] = read.astype(mixed.dtype)

    weights.wait()

    def e1(c, r):
        jj = at(j, r, B)
        return remote(part.at[2 * c, :, jj], r1e.at[c, r - 1], e1s.at[c, r], e1r.at[c, r], dp=i * B + jj)

    def o1(c, r):
        ii = at(i, r, A)
        return remote(part.at[2 * c + 1, ii], r1o.at[c, r - 1], o1s.at[c, r], o1r.at[c, r], dp=ii * B + j)

    def e2(c, r):
        ii = at(i, r, A)
        return remote(s2e.at[c, ii], r2e.at[c, r - 1], e2s.at[c, r], e2r.at[c, r], dp=ii * B + j)

    def o2(c, r):
        jj = at(j, r, B)
        return remote(s2o.at[c, jj], r2o.at[c, r - 1], o2s.at[c, r], o2r.at[c, r], dp=i * B + jj)

    @pl.loop(0, half)
    def _(c):
        for odd in range(2):
            columns = pl.ds(pl.multiple_of((2 * c + odd) * C, C), C)

            @pl.loop(0, ND)
            def _(s):
                block = jnp.dot(mixed[s], w[:, columns], preferred_element_type=jnp.float32)
                part[2 * c + odd, lax.div(s, B), lax.rem(s, B)] = block.astype(part.dtype)

            for r in range(1, A if odd else B):
                (o1 if odd else e1)(c, r).start()

    @pl.loop(0, half)
    def _(c):
        for r in range(1, B):
            e1(c, r).wait_recv()
        for r in range(A):
            ii = at(i, r, A)
            total = part[2 * c, ii, j].astype(jnp.float32)
            for k in range(1, B):
                total += r1e[c, k - 1, ii].astype(jnp.float32)
            if r:
                s2e[c, ii] = total.astype(s2e.dtype)
                e2(c, r).start()
            else:
                keep[2 * c] = total
        for r in range(1, A):
            o1(c, r).wait_recv()
        for r in range(B):
            jj = at(j, r, B)
            total = part[2 * c + 1, i, jj].astype(jnp.float32)
            for k in range(1, A):
                total += r1o[c, k - 1, jj].astype(jnp.float32)
            if r:
                s2o[c, jj] = total.astype(s2o.dtype)
                o2(c, r).start()
            else:
                keep[2 * c + 1] = total

    @pl.loop(0, half)
    def _(c):
        for odd, n, copies, slots in ((0, A, e2, r2e), (1, B, o2, r2o)):
            total = keep[2 * c + odd]
            for r in range(1, n):
                copies(c, r).wait_recv()
                total += slots[c, r - 1].astype(jnp.float32)
            columns = pl.ds(pl.multiple_of((2 * c + odd) * C, C), C)
            out_ref[:, columns] = total.astype(out_ref.dtype)

    for r in range(1, ND):
        queries[r].wait_send()
    for copy in list(first.values()) + list(second.values()):
        copy.wait_send()

    @pl.loop(0, half)
    def _(c):
        for r in range(1, B):
            e1(c, r).wait_send()
            o2(c, r).wait_send()
        for r in range(1, A):
            o1(c, r).wait_send()
            e2(c, r).wait_send()


def split_of(n):
    for a in range(int(n**0.5), 0, -1):
        if n % a == 0:
            return a, n // a


def kernel_body(query_rows, key_rows, value_rows, out_weight):
    ND, NS = lax.axis_size("dp"), lax.axis_size("sp")
    _, T, H, size = query_rows.shape
    V, rows = out_weight.shape[1], out_weight.shape[0]
    A, B = split_of(ND)
    HD, HS, NC = H // ND, H // ND // NS, 16
    C, half, count = V // NC, NC // 2, T * NS
    key_feature = feature_map(key_rows)
    state = jnp.einsum(
        "bthd,bthe->bhed", key_feature, value_rows, preferred_element_type=jnp.float32
    )[0] / count
    mass = jnp.sum(key_feature.astype(jnp.float32), axis=1)[0] / count
    mass = jnp.broadcast_to(mass[:, None, :].astype(jnp.bfloat16), (H, EXTRA, size))
    state = jnp.concatenate([state.astype(jnp.bfloat16), mass], axis=1).reshape(ND, NS, HS, size + EXTRA, size)
    query = query_rows.reshape(T * H, size)
    bf, block = jnp.bfloat16, (HS, size + EXTRA, size)
    dma = pltpu.SemaphoreType.DMA
    out = pl.pallas_call(
        functools.partial(kernel, ND, NS, A, B, count),
        out_shape=jax.ShapeDtypeStruct((T, V), bf),
        in_specs=[
            pl.BlockSpec(memory_space=pl.ANY),
            pl.BlockSpec(memory_space=pltpu.VMEM),
            pl.BlockSpec(memory_space=pl.ANY),
        ],
        out_specs=pl.BlockSpec(memory_space=pltpu.VMEM),
        scratch_shapes=[
            pltpu.VMEM((T * H, size), bf),
            pltpu.VMEM((T * H, size), jnp.float32),
            pltpu.VMEM((ND, HD, T, size), bf),
            pltpu.VMEM((rows, V), bf),
            pltpu.VMEM((ND, HD, T, size), bf),
            pltpu.VMEM((NS - 1, ND) + block, bf),
            pltpu.VMEM((ND,) + block, bf),
            pltpu.VMEM((ND, NS) + block, bf),
            pltpu.VMEM((ND, T, HD * size), bf),
            pltpu.VMEM((NC, A, B, T, C), bf),
            pltpu.VMEM((half, B - 1, A, T, C), bf),
            pltpu.VMEM((half, A - 1, B, T, C), bf),
            pltpu.VMEM((half, A, T, C), bf),
            pltpu.VMEM((half, B, T, C), bf),
            pltpu.VMEM((NC, T, C), jnp.float32),
            pltpu.VMEM((half, A - 1, T, C), bf),
            pltpu.VMEM((half, B - 1, T, C), bf),
            dma, dma, dma((2,)), dma((ND,)), dma((ND,)), dma((ND, NS)), dma((ND, NS)), dma((ND, NS)), dma((ND, NS)),
            dma((half, B)), dma((half, B)), dma((half, A)), dma((half, A)),
            dma((half, A)), dma((half, A)), dma((half, B)), dma((half, B)),
        ],
        compiler_params=pltpu.CompilerParams(
            collective_id=0, has_side_effects=True, vmem_limit_bytes=63 * 2**20
        ),
    )(query, state, out_weight)
    return out[None]


def body(query_rows, key_rows, value_rows, out_weight):
    ND, NS = lax.axis_size("dp"), lax.axis_size("sp")
    batch, T, H, size = query_rows.shape
    rows, V = out_weight.shape
    need = 2 * rows * V + 2 * ND * T * V * 2 + 2 * T * V * 8 + 6 * H * T * size * 2
    fits = batch == 1 and H % (ND * NS) == 0 and V % 2048 == 0 and min(split_of(ND)) > 1
    fits = fits and size == 128 and T % 16 == 0 and T * H % 1024 == 0 and NS & (NS - 1) == 0 and need < 56 * 2**20
    run = kernel_body if fits else plain_body
    return run(query_rows, key_rows, value_rows, out_weight)


def solution(mesh):
    placed = (
        P(("shift", "dp"), "sp", None, None),
        P(("shift", "dp"), "sp", None, None),
        P(("shift", "dp"), "sp", None, None),
        P(("shift", "dp"), None),
    )
    return jax.shard_map(
        body, mesh=mesh, in_specs=placed, out_specs=P(("shift", "dp"), "sp", None), check_vma=False
    )
```
